128 devices in a mesh: shard: 32 (over y, x, core), tp: 4 (over z).
Axes of the slice: x: 4, y: 4, z: 4, core: 2. Of those that a mesh axis runs over, the one named last changes fastest.
Arguments:
- weight_gate: bfloat16 [2560, 9728], P('shard', 'tp'), may hold values from -0.21875 to 0.21875
- low_gate: bfloat16 [2560, 32], P('shard'), may hold values from -0.125 to 0.125
- high_gate: bfloat16 [32, 9728], P(None, 'tp'), may hold values from -1 to 1
- weight_up: bfloat16 [2560, 9728], P('shard', 'tp'), may hold values from -0.21875 to 0.21875
- low_up: bfloat16 [2560, 32], P('shard'), may hold values from -0.125 to 0.125
- high_up: bfloat16 [32, 9728], P(None, 'tp'), may hold values from -1 to 1
- norm_gain: float32 [2560], P('shard'), may hold values from 0.25 to 1.75
Outputs:
- ready_gate: bfloat16 [2560, 9728], P(None, 'tp')
- ready_up: bfloat16 [2560, 9728], P(None, 'tp')
- factor_gate: float32 [9728], P('tp')
- factor_up: float32 [9728], P('tp')
The draws below stay inside these ranges and needn't reach their ends.
All inputs are finite; a program needn't handle non-finite values.
Results may differ from the reference program's by a relative error of at most 0.001.
Values may be sent and summed in bfloat16 or wider, within the bound.
A program may use at most 128 MiB of HBM per device.

```python
import jax
import jax.numpy as jnp
from jax import lax

D_MODEL = 2560
D_INNER = 9728
RANK = 32


def spiked(result, rng, source, target, shards_of, factor):
    owner, partner = [(jnp.arange(result.shape[dim]) // (result.shape[dim] // shards_of)).reshape([-1 if axis == dim else 1 for axis in range(result.ndim)]) for dim in (source, target)]
    chosen = jax.random.permutation(rng, shards_of)[partner]
    strong = (owner == chosen) | (owner == (partner + shards_of // 2) % shards_of)
    return jnp.where(strong, factor * result, result)


def block_scale(stream_key, dims, split, low, largest):
    loudness, own = 1.0, jax.random.fold_in(stream_key, 6)
    for position, shards_of in split:
        draws = jnp.exp(jax.random.uniform(jax.random.fold_in(own, position), (shards_of,), jnp.float32, low / len(split), largest / len(split)))
        loudness = loudness * jnp.repeat(draws, dims[position] // shards_of).reshape([-1 if axis == position else 1 for axis in range(len(dims))])
    return loudness


def scatter_about(rng, shape, scale, most, shards=(), dtype=jnp.bfloat16):
    drawn = jax.random.normal(rng, shape, jnp.float32) * scale
    if len(shards) > 0:
        drawn = block_scale(rng, shape, shards, -0.22, 0.18) * drawn
    return jnp.clip(drawn, min=-most, max=most).astype(dtype)


def bell_draw_with(key, shape, scale, bound, shards, heavy, kind=jnp.bfloat16):
    array = scale * jax.random.normal(key, shape, jnp.float32)
    if shards:
        array = array * block_scale(key, shape, shards, -0.22, 0.18)
    return jnp.clip(spiked(array, jax.random.fold_in(key, 3), *heavy), -bound, bound).astype(kind)


def setup_inputs(seed: int = 0) -> dict:
    streams_of = jax.random.split(jax.random.key(seed), 8)
    return {
        "weight_gate": bell_draw_with(streams_of[0], (D_MODEL, D_INNER), D_MODEL ** -0.5, 0.21875, ((0, 32), (1, 4)), (0, 1, 32, 2.75)),
        "low_gate": scatter_about(streams_of[1], (D_MODEL, RANK), D_MODEL ** -0.5, 0.125, ((0, 32),)),
        "high_gate": scatter_about(streams_of[2], (RANK, D_INNER), RANK ** -0.5, 1.0, ((1, 4),)),
        "weight_up": bell_draw_with(streams_of[3], (D_MODEL, D_INNER), D_MODEL ** -0.5, 0.21875, ((0, 32), (1, 4)), (0, 1, 32, 2.75)),
        "low_up": scatter_about(streams_of[4], (D_MODEL, RANK), D_MODEL ** -0.5, 0.125, ((0, 32),)),
        "high_up": scatter_about(streams_of[5], (RANK, D_INNER), RANK ** -0.5, 1.0, ((1, 4),)),
        "norm_gain": jnp.clip(1.0 + 0.15 * jax.random.normal(streams_of[6], (D_MODEL,), jnp.float32), 0.25, 1.75),
    }


mix_rate = 2.0

def reference(weight_gate, low_gate, high_gate, weight_up, low_up, high_up, norm_gain):
    latest_gate = weight_gate.astype(jnp.float32) + mix_rate * jnp.dot(low_gate, high_gate, preferred_element_type=jnp.float32)
    latest_up = weight_up.astype(jnp.float32) + mix_rate * jnp.dot(low_up, high_up, preferred_element_type=jnp.float32)
    latest_gained_gate = latest_gate * norm_gain[:, None]
    latest_gained_up = latest_up * norm_gain[:, None]
    factor_gate = jnp.sqrt(lax.optimization_barrier(jnp.sum(latest_gained_gate * latest_gained_gate, axis=0)))
    ready_gate = (latest_gained_gate / factor_gate).astype(jnp.bfloat16)
    factor_up = jnp.sqrt(lax.optimization_barrier(jnp.sum(latest_gained_up * latest_gained_up, axis=0)))
    ready_up = (latest_gained_up / factor_up).astype(jnp.bfloat16)
    return (ready_gate, ready_up, factor_gate, factor_up)
```

```python
import functools

import jax
import jax.numpy as jnp
from jax import lax
from jax.experimental import pallas as pl
from jax.experimental.pallas import tpu as pltpu
from jax.sharding import PartitionSpec as P

MESH = pl.DeviceIdType.MESH
SIDE = 4
BLOCKS = 32
ROWS = 80
HALF = 40
WIDE = 2432
PACK = 128
LINKS = ((0, 1), (0, -1), (1, 1), (1, -1))
ITEMS = 11


def schedule(axis, sign):
    first, second = axis, 1 - axis
    half = 0 if sign == 1 else 1

    def at(along, across):
        return (along, across) if axis == 0 else (across, along)

    return [
        (first, at(0, 0), None),
        (second, at(0, 0), None),
        (first, at(-sign, 0), half),
        (second, at(0, -1), None),
        (second, at(0, 1), None),
        (second, at(-sign, 0), half),
        (second, at(0, 2), half),
        (second, at(0, 2), 1 - half),
        (second, at(-sign, -1), half),
        (second, at(-sign, 1), half),
        (second, at(-sign, 2), half),
    ]


RELEASE = {1: (3, 4, 5), 2: (6,), 3: (7, 8), 4: (9,), 5: (10,), 7: (11,)}


def gather_kernel(
    wg_ref, wu_ref, pk_ref, og_ref, ou_ref,
    own_sem, send_sem, recv_sem, cross_send, cross_recv,
):
    shard = lax.axis_index("shard")
    core = lax.rem(shard, 2)
    chip = shard // 2
    y, x = chip // SIDE, lax.rem(chip, SIDE)
    a = x + core * (y - x)
    b = y + core * (x - y)
    ma, mb = 1 + 3 * core, 4 - 3 * core

    def block(da, db):
        ca = lax.rem(a + da + SIDE, SIDE)
        cb = lax.rem(b + db + SIDE, SIDE)
        return (ca * ma + cb * mb) * 2 + core

    own = block(0, 0)
    partner = own + 1 - 2 * core
    near = [block(sign, 0) if axis == 0 else block(0, sign) for axis, sign in LINKS]

    copies = [
        pltpu.make_async_copy(wg_ref, og_ref.at[own, :, pl.ds(0, WIDE)], own_sem.at[0]),
        pltpu.make_async_copy(pk_ref, og_ref.at[own, :, pl.ds(WIDE, PACK)], own_sem.at[1]),
        pltpu.make_async_copy(wu_ref, ou_ref.at[own], own_sem.at[2]),
    ]
    for c in copies:
        c.start()
    barrier = pltpu.get_barrier_semaphore()
    for other in near + [partner]:
        pl.semaphore_signal(barrier, inc=1, device_id={"shard": other}, device_id_type=MESH)
    pl.semaphore_wait(barrier, 5)
    for c in copies:
        c.wait()

    outs = (og_ref, ou_ref)

    def piece(array, place, half):
        ref = outs[array].at[block(*place)]
        if half is not None:
            ref = ref.at[pl.ds(half * HALF, HALF)]
        return ref

    plans = [schedule(axis, sign) for axis, sign in LINKS]

    def link_copy(link, item):
        array, place, half = plans[link][item]
        ref = piece(array, place, half)
        return pltpu.make_async_remote_copy(
            src_ref=ref, dst_ref=ref,
            send_sem=send_sem.at[link, item], recv_sem=recv_sem.at[link, item],
            device_id={"shard": near[link]}, device_id_type=MESH,
        )

    def arrived(link, item):
        axis, sign = LINKS[link]
        array, (da, db), half = plans[link][item]
        place = (da - sign, db) if axis == 0 else (da, db - sign)
        return array, place, half

    def arrival(link, item):
        ref = piece(*arrived(link, item))
        return pltpu.make_async_remote_copy(
            src_ref=ref, dst_ref=ref,
            send_sem=send_sem.at[link, item], recv_sem=recv_sem.at[link, item],
            device_id={"shard": near[link]}, device_id_type=MESH,
        )

    def cross(slot, ref):
        return pltpu.make_async_remote_copy(
            src_ref=ref, dst_ref=ref,
            send_sem=cross_send.at[slot], recv_sem=cross_recv.at[slot],
            device_id={"shard": partner}, device_id_type=MESH,
        )

    for item in (0, 1):
        for link in range(4):
            link_copy(link, item).start()
    crosses = []

    def hand_over(ref, mirror):
        c = cross(len(crosses), ref)
        c.start()
        crosses.append((c, cross(len(crosses), mirror)))

    def mirror_piece(array, place, half):
        da, db = place
        ca = lax.rem(b + da + SIDE, SIDE)
        cb = lax.rem(a + db + SIDE, SIDE)
        index = (ca * mb + cb * ma) * 2 + 1 - core
        ref = outs[array].at[index]
        if half is not None:
            ref = ref.at[pl.ds(half * HALF, HALF)]
        return ref

    for array in (0, 1):
        hand_over(piece(array, (0, 0), None), mirror_piece(array, (0, 0), None))
    for item in range(ITEMS):
        for link in range(4):
            arrival(link, item).wait_recv()
            hand_over(piece(*arrived(link, item)), mirror_piece(*arrived(link, item)))
        for late in RELEASE.get(item + 1, ()):
            for link in range(4):
                link_copy(link, late - 1).start()
    for item in range(ITEMS):
        for link in range(4):
            link_copy(link, item).wait_send()
    for sent, got in crosses:
        sent.wait_send()
        got.wait_recv()


def gather(wg, wu, pk):
    slots = 2 + 4 * ITEMS
    return pl.pallas_call(
        gather_kernel,
        name="torus_gather",
        out_shape=(
            pltpu.VMEM((BLOCKS, ROWS, WIDE + PACK), jnp.bfloat16),
            pltpu.VMEM((BLOCKS, ROWS, WIDE), jnp.bfloat16),
        ),
        in_specs=[pl.BlockSpec(memory_space=pl.ANY)] * 3,
        out_specs=(pl.BlockSpec(memory_space=pltpu.VMEM),) * 2,
        scratch_shapes=[
            pltpu.SemaphoreType.DMA((3,)),
            pltpu.SemaphoreType.DMA((4, ITEMS)),
            pltpu.SemaphoreType.DMA((4, ITEMS)),
            pltpu.SemaphoreType.DMA((slots,)),
            pltpu.SemaphoreType.DMA((slots,)),
        ],
        compiler_params=pltpu.CompilerParams(
            collective_id=0, has_side_effects=True, vmem_limit_bytes=2 << 20
        ),
    )(wg, wu, pk)


TILE = 256
CHUNK = 160
TOTAL = BLOCKS * ROWS


def finish_kernel(og_ref, ou_ref, hg_ref, hu_ref, rg_ref, ru_ref, fg_ref, fu_ref,
                  gain, gained, out, sem):
    lanes = lax.broadcasted_iota(jnp.int32, (PACK, 128), 0)
    pick = jnp.where((lanes >= 64) & (lanes < 67), 1.0, 0.0).astype(jnp.bfloat16)
    for r in range(0, TOTAL, 320):
        gain[pl.ds(r, 320)] = jnp.dot(
            og_ref[pl.ds(r, 320), pl.ds(WIDE, PACK)], pick, preferred_element_type=jnp.float32
        )
    none = jnp.zeros((32, 128), jnp.bfloat16)

    def halves(parts):
        rhs, refs = [], []
        for array, at in parts:
            at = pl.ds(at, 128)
            if array == 0:
                rhs.append(jnp.concatenate([hg_ref[:, at], none], axis=0))
                refs.append(og_ref.at[:, at])
            else:
                rhs.append(jnp.concatenate([none, hu_ref[:, at]], axis=0))
                refs.append(ou_ref.at[:, at])
        return jnp.concatenate(rhs, axis=1), refs

    def write(slot, parts):
        for half, (array, at) in enumerate(parts):
            dst = (rg_ref, ru_ref)[array].at[:, pl.ds(at, 128)]
            yield pltpu.make_async_copy(out.at[slot, half], dst, sem.at[slot, half])

    def tile(slot, parts):
        rhs, refs = halves(parts)
        acc = jnp.zeros((8, TILE), jnp.float32)
        for r in range(0, TOTAL, CHUNK):
            rows = pl.ds(r, CHUNK)
            d = jnp.dot(og_ref[rows, pl.ds(WIDE, 64)], rhs, preferred_element_type=jnp.float32)
            w = jnp.concatenate([ref[rows].astype(jnp.float32) for ref in refs], axis=1)
            g = gain[rows]
            v = (w + d) * jnp.concatenate([g, g], axis=1)
            gained[rows] = v
            acc = acc + jnp.sum((v * v).reshape(CHUNK // 8, 8, TILE), axis=0)
        total = jnp.sum(acc, axis=0, keepdims=True)
        factor = jnp.sqrt(total)
        inverse = 1.0 / factor
        for half, (array, at) in enumerate(parts):
            (fg_ref, fu_ref)[array][:, pl.ds(at, 128)] = factor[:, half * 128:half * 128 + 128]
        for r in range(0, TOTAL, CHUNK):
            rows = pl.ds(r, CHUNK)
            v = (gained[rows] * inverse).astype(jnp.bfloat16)
            out[slot, 0, rows] = v[:, :128]
            out[slot, 1, rows] = v[:, 128:]
        for c in write(slot, parts):
            c.start()

    def gate_parts(t):
        at = pl.multiple_of(t * TILE, TILE)
        return ((0, at), (0, at + 128))

    def up_parts(t):
        at = pl.multiple_of(t * TILE + 128, 128)
        return ((1, at), (1, pl.multiple_of(at + 128, 128)))

    def wait(slot, parts):
        for c in write(slot, parts):
            c.wait()

    def gate_step(t, carry):
        slot = lax.rem(t, 2)

        @pl.when(t >= 2)
        def _():
            wait(slot, gate_parts(t - 2))

        tile(slot, gate_parts(t))
        return carry

    lax.fori_loop(0, 9, gate_step, 0)
    middle = ((0, 9 * TILE), (1, 0))
    wait(1, gate_parts(7))
    tile(1, middle)

    def up_step(t, carry):
        slot = lax.rem(t, 2)

        @pl.when(t == 0)
        def _():
            wait(0, gate_parts(8))

        @pl.when(t == 1)
        def _():
            wait(1, middle)

        @pl.when(t >= 2)
        def _():
            wait(slot, up_parts(t - 2))

        tile(slot, up_parts(t))
        return carry

    lax.fori_loop(0, 9, up_step, 0)
    wait(1, up_parts(7))
    wait(0, up_parts(8))


def finish(og, ou, hg, hu):
    return pl.pallas_call(
        finish_kernel,
        name="merge_and_scale",
        out_shape=(
            jax.ShapeDtypeStruct((TOTAL, WIDE), jnp.bfloat16),
            jax.ShapeDtypeStruct((TOTAL, WIDE), jnp.bfloat16),
            jax.ShapeDtypeStruct((1, WIDE), jnp.float32),
            jax.ShapeDtypeStruct((1, WIDE), jnp.float32),
        ),
        in_specs=[pl.BlockSpec(memory_space=pltpu.VMEM)] * 4,
        out_specs=(
            pl.BlockSpec(memory_space=pl.ANY),
            pl.BlockSpec(memory_space=pl.ANY),
            pl.BlockSpec(memory_space=pltpu.VMEM),
            pl.BlockSpec(memory_space=pltpu.VMEM),
        ),
        scratch_shapes=[
            pltpu.VMEM((TOTAL, 128), jnp.float32),
            pltpu.VMEM((TOTAL, TILE), jnp.float32),
            pltpu.VMEM((2, 2, TOTAL, 128), jnp.bfloat16),
            pltpu.SemaphoreType.DMA((2, 2)),
        ],
        compiler_params=pltpu.CompilerParams(vmem_limit_bytes=16 << 20),
    )(og, ou, hg, hu)


def packed(low_gate, low_up, gain):
    def cut(v):
        return lax.reduce_precision(v, 8, 7)

    high = cut(gain)
    mid = cut(gain - high)
    low = gain - high - mid
    parts = [2.0 * low_gate.astype(jnp.float32), 2.0 * low_up.astype(jnp.float32)]
    parts += [v[:, None] for v in (high, mid, low)]
    parts.append(jnp.zeros((ROWS, PACK - 67), jnp.float32))
    return jnp.concatenate(parts, axis=1).astype(jnp.bfloat16)


def local(weight_gate, low_gate, high_gate, weight_up, low_up, high_up, norm_gain):
    pk = packed(low_gate, low_up, norm_gain)
    og, ou = gather(weight_gate, weight_up, pk)
    ready_gate, ready_up, factor_gate, factor_up = finish(
        og.reshape(TOTAL, WIDE + PACK), ou.reshape(TOTAL, WIDE), high_gate, high_up
    )
    return ready_gate, ready_up, factor_gate.reshape(WIDE), factor_up.reshape(WIDE)


def solution(mesh):
    in_specs = (
        P("shard", "tp"),
        P("shard", None),
        P(None, "tp"),
        P("shard", "tp"),
        P("shard", None),
        P(None, "tp"),
        P("shard"),
    )
    out_specs = (P(None, "tp"), P(None, "tp"), P("tp"), P("tp"))
    return jax.shard_map(local, mesh=mesh, in_specs=in_specs, out_specs=out_specs, check_vma=False)
```
